32 devices in a mesh: px: 2 (over core), pz: 16 (over z, y, x).
Axes of the slice: x: 2, y: 2, z: 4, core: 2. Of those that a mesh axis runs over, the one named last changes fastest.
Arguments:
- velocity: float32 [3, 256, 32, 256], P(None, 'pz', None, 'px'), may hold values from -8 to 8, as said below
- filter_inverse: float32 [256, 256], replicated, may hold values from 0 to 2, as said below
- filter_block: int32 [256], replicated, may hold values from 0 to 7, never falling along the last dimension, each value on 1 to 128 neighbouring positions
- plane_bin: int32 [256], replicated, may hold values from 0 to 63, never falling along the last dimension, each value on 1 to 16 neighbouring positions
Outputs:
- leonard: float32 [6, 256, 32, 256], P(None, 'pz', None, 'px')
- viscosity: float32 [256, 32, 256], P('pz', None, 'px')
- coefficient: float32 [256], replicated
The draws below stay inside these ranges and needn't reach their ends.
Inputs may be any that keep to these rules, and one draw needn't show every extreme that they name: `velocity`: each component is a rough random field. `filter_inverse`: entries are positive. `filter_block`: never falls along the planes; each of the 8 blocks holds 1 to 128 consecutive planes, one exactly 128. `plane_bin`: never falls along the planes; each of the 64 bins holds 1 to 16 consecutive planes, one exactly 16.
All inputs are finite; a program needn't handle non-finite values.
Results may differ from the reference program's by a relative error of at most 0.0003.
Values sent between devices are 32-bit elements; how exact they have to be, the bound alone decides.
No kernel may reach another device: no remote copies, remote signals or barrier semaphores. Data moves between devices by JAX's collectives and lax.ppermute only.
A program may use at most 128 MiB of HBM per device.

```python
import math
import jax
import jax.numpy as jnp
import numpy as np
from jax import lax

NY = 256
NFB = 8
FBMOST = 128
NBIN = 64
BINMOST = 16
NX = 256
NZ = 32


def draw_velocity(key, part):
    noise_key, scale_key = jax.random.split(jax.random.fold_in(key, 11))
    base = jax.random.normal(noise_key, (3, NY, NZ, NX), jnp.float32)
    amplitude = jnp.exp(jax.random.uniform(scale_key, (1, 1, NZ, NX // 8), jnp.float32, -0.7, 0.7))
    amplitude = jnp.repeat(amplitude, 8, axis=3)
    return jnp.clip(base * amplitude, -8.0, 8.0)


def draw_filter_inverse(key, part):
    entry_key = jax.random.fold_in(key, 23)
    rows = jnp.arange(NY, dtype=jnp.float32)
    distance = jnp.abs(rows[:, None] - rows[None, :])
    factors = jax.random.uniform(entry_key, (NY, NY), jnp.float32, 0.5, 1.5)
    return jnp.exp(-distance / 256.0) * factors


def split_up(number_of, total, bound, slope):
    loads = [(1 << 20) // math.isqrt(grade ** slope) + 1 for grade in range(2, number_of + 1)]
    spare, holding = total - bound - (number_of - 1), [1] * (number_of - 1)
    while spare > 0:
        free = [i for i in range(number_of - 1) if holding[i] < bound]
        whole, budget = sum([loads[i] for i in free]), spare
        for i in free:
            extra = min(bound - holding[i], max(1, budget * loads[i] // whole), spare)
            holding[i] = holding[i] + extra
            spare = spare - extra
    return np.array([bound] + holding)


def ragged_sizes(rng, count, total, reach, lean):
    if count == 2:
        one = jax.random.randint(rng, (), max(1, total - reach), min(reach, total - 1) + 1)
        return jnp.stack([one, total - one])
    sizes = jnp.asarray(split_up(count, total, reach, lean), jnp.int32)
    couples = (count - 1) // 2
    donor, sink = sizes[1:1 + 2 * couples:2], sizes[2:2 + 2 * couples:2]
    room = jnp.minimum(donor - 1, reach - sink)
    shifted = jax.random.randint(jax.random.fold_in(rng, 1), (couples,), 0, 1 << 20) % (room + 1)
    sizes = sizes.at[1:1 + 2 * couples:2].set(donor - shifted).at[2:2 + 2 * couples:2].set(sink + shifted)
    return sizes[jax.random.permutation(jax.random.fold_in(rng, 2), count)]


def setup_inputs(seed: int = 0) -> dict:
    keys = jax.random.split(jax.random.key(seed), 5)
    velocity = draw_velocity(jax.random.fold_in(keys[4], 71), 0)
    filter_inverse = draw_filter_inverse(jax.random.fold_in(keys[4], 71), 0)
    filter_block = jnp.searchsorted(jnp.cumsum(ragged_sizes(keys[2], NFB, NY, FBMOST, 1)), jnp.arange(NY), side="right").astype(jnp.int32)
    plane_bin = jnp.searchsorted(jnp.cumsum(ragged_sizes(keys[3], NBIN, NY, BINMOST, 1)), jnp.arange(NY), side="right").astype(jnp.int32)
    return dict(velocity=velocity, filter_inverse=filter_inverse, filter_block=filter_block, plane_bin=plane_bin)


def block_weights(filter_inverse, filter_block):
    same = (filter_block[:, None] == filter_block[None, :]).astype(jnp.float32)
    masked = filter_inverse * same
    return masked / lax.optimization_barrier(jnp.sum(masked, axis=1, keepdims=True))

def quantities(padded):
    centre = padded[:, 1:-1, 1:-1, 1:-1]
    along_y = (padded[:, 2:, 1:-1, 1:-1] - padded[:, :-2, 1:-1, 1:-1]) * 0.5
    along_z = (padded[:, 1:-1, 2:, 1:-1] - padded[:, 1:-1, :-2, 1:-1]) * 0.5
    along_x = (padded[:, 1:-1, 1:-1, 2:] - padded[:, 1:-1, 1:-1, :-2]) * 0.5
    strain = jnp.stack([along_x[0], along_y[1], along_z[2], 0.5 * (along_y[0] + along_x[1]), 0.5 * (along_z[0] + along_x[2]), 0.5 * (along_z[1] + along_y[2])])
    magnitude = jnp.sqrt(2.0 * lax.optimization_barrier(jnp.sum(strain[:3] * strain[:3], axis=0)) + 4.0 * lax.optimization_barrier(jnp.sum(strain[3:] * strain[3:], axis=0)))
    products = jnp.stack([centre[0] * centre[0], centre[1] * centre[1], centre[2] * centre[2], centre[0] * centre[1], centre[0] * centre[2], centre[1] * centre[2]])
    fields = jnp.concatenate([centre, strain, products, magnitude[None] * strain], axis=0)
    along = (fields[..., :-2] + 2.0 * fields[..., 1:-1] + fields[..., 2:]) * 0.25
    boxed = (along[:, :, :-2] + 2.0 * along[:, :, 1:-1] + along[:, :, 2:]) * 0.25
    return (boxed, magnitude[:, 1:-1, 1:-1])

def contract(filtered):
    speed = filtered[0:3]
    strain = filtered[3:9]
    products = filtered[9:15]
    scaled = filtered[15:21]
    leonard = products - jnp.stack([speed[0] * speed[0], speed[1] * speed[1], speed[2] * speed[2], speed[0] * speed[1], speed[0] * speed[2], speed[1] * speed[2]])
    fmag = jnp.sqrt(2.0 * lax.optimization_barrier(jnp.sum(strain[:3] * strain[:3], axis=0)) + 4.0 * lax.optimization_barrier(jnp.sum(strain[3:] * strain[3:], axis=0)))
    model = scaled - 4.0 * fmag[None] * strain
    weights = jnp.array([1.0, 1.0, 1.0, 2.0, 2.0, 2.0], jnp.float32).reshape(6, 1, 1, 1)
    product_lm = lax.optimization_barrier(jnp.sum(weights * leonard * model, axis=0))
    product_mm = lax.optimization_barrier(jnp.sum(weights * model * model, axis=0))
    return (leonard, product_lm, product_mm)

def reference(velocity, filter_inverse, filter_block, plane_bin):
    weights = block_weights(filter_inverse, filter_block)

    def one_plane(plane):
        indices = ((plane + jnp.arange(-2, 3, dtype=jnp.int32)) % NZ).astype(jnp.int32)
        window = jnp.take(velocity, indices, axis=2)
        window = jnp.pad(window, ((0, 0), (1, 1), (0, 0), (0, 0)))
        window = jnp.concatenate([window[..., -2:], window, window[..., :2]], axis=3)
        boxed, magnitude = quantities(window)
        filtered = jnp.einsum('ab,kbzx->kazx', weights, boxed, precision=lax.Precision.HIGHEST)
        leonard, product_lm, product_mm = contract(filtered)
        return (leonard[:, :, 0, :], lax.optimization_barrier(jnp.sum(product_lm, axis=(1, 2))), lax.optimization_barrier(jnp.sum(product_mm, axis=(1, 2))), magnitude[:, 0, :])
    leonard, plane_lm, plane_mm, magnitude = lax.map(one_plane, jnp.arange(NZ, dtype=jnp.int32))
    plane_lm = lax.optimization_barrier(jnp.sum(plane_lm, axis=0))
    plane_mm = lax.optimization_barrier(jnp.sum(plane_mm, axis=0))
    onehot = (plane_bin[:, None] == jnp.arange(NBIN, dtype=jnp.int32)[None, :]).astype(jnp.float32)
    numer = jnp.dot(plane_lm, onehot, precision=lax.Precision.HIGHEST)
    denom = jnp.dot(plane_mm, onehot, precision=lax.Precision.HIGHEST)
    per_bin = numer / jnp.maximum(denom, jnp.float32(NX * NZ))
    coefficient = jnp.dot(onehot, per_bin, precision=lax.Precision.HIGHEST)
    leonard = jnp.transpose(leonard, (1, 2, 0, 3))
    viscosity = coefficient[:, None, None] * jnp.transpose(magnitude, (1, 0, 2))
    return (leonard, viscosity, coefficient)
```

```python
import functools

import jax
import jax.numpy as jnp
from jax import lax
from jax.experimental import pallas as pl
from jax.experimental.pallas import tpu as pltpu
from jax.sharding import PartitionSpec as P

NBIN = 64
LANES = 128
F32 = jnp.float32
BF16 = jnp.bfloat16
PAIRS = ((0, 0), (1, 1), (2, 2), (0, 1), (0, 2), (1, 2))


def vmem(n):
    return [pl.BlockSpec(memory_space=pltpu.VMEM)] * n


def iota(shape, dim):
    return lax.broadcasted_iota(jnp.int32, shape, dim)


def swap_chunks(t, nz):
    group = LANES // nz
    rows, cols = t.shape
    row, lane = iota(t.shape, 0), iota(t.shape, 1)
    bit = group // 2
    while bit:
        up = pltpu.roll(pltpu.roll(t, bit * nz, 1), rows - bit, 0)
        down = pltpu.roll(pltpu.roll(t, cols - bit * nz, 1), bit, 0)
        rbit = (row // bit) % 2
        lbit = (lane // (bit * nz)) % 2
        t = jnp.where(rbit == lbit, t, jnp.where(rbit == 0, up, down))
        bit //= 2
    return t


def swap_rows(ts, nz):
    group = LANES // nz
    ts = list(ts)
    rows = ts[0].shape[0]
    row = iota(ts[0].shape, 0)
    bit = len(ts) // 2
    while bit:
        low = (row // (bit * group)) % 2 == 0
        for g in range(len(ts)):
            if not g & bit:
                a, b = ts[g], ts[g | bit]
                ts[g] = jnp.where(low, a, pltpu.roll(b, bit * group, 0))
                ts[g | bit] = jnp.where(low, pltpu.roll(a, rows - bit * group, 0), b)
        bit //= 2
    return ts


def tiles_kernel(nz, vel_ref, out_ref, edge_ref):
    group = LANES // nz
    nl = 8 // group
    planes = vel_ref.shape[1]
    for f in range(3):
        for k in range(planes // 8):
            ts = []
            for g in range(nl):
                p0 = 8 * k + g * group
                v = vel_ref[f, p0 : p0 + group].reshape(LANES, LANES)
                ts.append(swap_chunks(v.T, nz))
            ts = swap_rows(ts, nz)
            r0 = f * planes + 8 * k
            for l in range(nl):
                t = ts[l].reshape(16, 8, LANES)
                out_ref[:, l, r0 : r0 + 8, :] = t
                if l == 0:
                    edge_ref[0, r0 : r0 + 8, :] = t[0]
                if l == nl - 1:
                    edge_ref[1, r0 : r0 + 8, :] = t[15]


def blocks_kernel(n, nz, me_ref, tiles_ref, next_ref, prev_ref, *outs):
    group = LANES // nz
    nt = LANES // group
    per = nt // n
    me = me_ref[0]
    rows = tiles_ref.shape[1]
    lane = iota((rows, LANES), 1)
    for m in range(n):
        d = me ^ m
        for i in range(per):
            outs[m][:, i * LANES : (i + 1) * LANES] = tiles_ref[per * d + i]
        after = jnp.minimum(per * d + per, nt - 1)
        before = jnp.maximum(per * d - 1, 0)
        right = jnp.where(d == n - 1, next_ref[...], tiles_ref[after])
        left = jnp.where(d == 0, prev_ref[...], tiles_ref[before])
        c0 = per * LANES
        if group == 4:
            outs[m][:, c0 : c0 + LANES] = jnp.where(lane < 2 * nz, right, left)
        else:
            outs[m][:, c0 : c0 + LANES] = right
            outs[m][:, c0 + LANES : c0 + 2 * LANES] = left


def split(x):
    hi = x.astype(BF16)
    lo = (x - hi.astype(F32)).astype(BF16)
    return hi, lo


def weights_kernel(inv_ref, col_ref, row_ref, w_ref, wd_ref):
    ny = inv_ref.shape[0]
    masked = jnp.where(col_ref[...] == row_ref[...], inv_ref[...], 0.0)
    w = masked / jnp.sum(masked, axis=1, keepdims=True)
    hi, lo = split(w)
    w_ref[0:ny] = hi
    w_ref[ny : 2 * ny] = lo
    lane = iota((ny, ny), 1)
    before = jnp.where(lane == 0, 0.0, pltpu.roll(w, 1, 1))
    after = jnp.where(lane == ny - 1, 0.0, pltpu.roll(w, ny - 1, 1))
    hi, lo = split(0.5 * (before - after))
    wd_ref[0:ny] = hi
    wd_ref[ny : 2 * ny] = lo


def shifts_z(v, nz):
    width = v.shape[1]
    z = iota(v.shape, 1) % nz
    below = jnp.where(z == 0, pltpu.roll(v, width - (nz - 1), 1), pltpu.roll(v, 1, 1))
    above = jnp.where(z == nz - 1, pltpu.roll(v, nz - 1, 1), pltpu.roll(v, width - 1, 1))
    return below, above


def shifts_x(v, nz):
    width = v.shape[1]
    return pltpu.roll(v, nz, 1), pltpu.roll(v, width - nz, 1)


def box(v, nz, width):
    before, after = shifts_x(v, nz)
    b = (before + 2.0 * v + after)[:, :width]
    below, above = shifts_z(b, nz)
    return (below + 2.0 * b + above) * 0.0625


def half_diff(pair):
    return 0.5 * (pair[1] - pair[0])


def norm_of(s):
    return jnp.sqrt(
        2.0 * (s[0] * s[0] + s[1] * s[1] + s[2] * s[2]) + 4.0 * (s[3] * s[3] + s[4] * s[4] + s[5] * s[5])
    )


def column_kernel(n, nz, width, me_ref, *refs):
    ins, refs = refs[:n], refs[n:]
    w_ref, wd_ref, bin_ref = refs[:3]
    outs, refs = refs[3 : 3 + n], refs[3 + n :]
    u_ref, uh, ul, xh, xl, fu, fd, fx, back = refs
    me = me_ref[0]
    ny = bin_ref.shape[0]
    planes = ny // n
    wide = u_ref.shape[2]
    per = width // LANES
    pad = 8
    chunk = 32

    for f in range(3):
        u_ref[f, 0:pad, :] = jnp.zeros((pad, wide), F32)
        u_ref[f, ny + pad : ny + 2 * pad, :] = jnp.zeros((pad, wide), F32)
    for m in range(n):
        row = pl.multiple_of((me ^ m) * planes, 8)
        for f in range(3):
            u_ref[f, pl.ds(pad + row, planes), :] = ins[m][f * planes : (f + 1) * planes, :]

    def fields(c, carry):
        r0 = pl.multiple_of(c * chunk, chunk)
        rows = pl.ds(r0, chunk)
        u, dx, dy, dz = [], [], [], []
        for f in range(3):
            ext = u_ref[f, pl.ds(r0, chunk + 2 * pad), :]
            v = ext[pad : pad + chunk]
            u.append(v)
            dy.append(0.5 * (ext[pad + 1 : pad + 1 + chunk] - ext[pad - 1 : pad - 1 + chunk]))
            dx.append(half_diff(shifts_x(v, nz)))
            dz.append(half_diff(shifts_z(v, nz)))
            hi, lo = split(box(v, nz, wide))
            uh[f, rows, :] = hi
            ul[f, rows, :] = lo
        s = (
            dx[0],
            dy[1],
            dz[2],
            0.5 * (dy[0] + dx[1]),
            0.5 * (dz[0] + dx[2]),
            0.5 * (dz[1] + dy[2]),
        )
        mag = norm_of(s)
        for i in range(per):
            back[i, 6, rows, :] = mag[:, i * LANES : (i + 1) * LANES]
        for k, (i, j) in enumerate(PAIRS):
            hi, lo = split(box(u[i] * u[j], nz, width))
            xh[k, rows, :] = hi
            xl[k, rows, :] = lo
            hi, lo = split(box(mag * s[k], nz, width))
            xh[6 + k, rows, :] = hi
            xl[6 + k, rows, :] = lo
        return carry

    lax.fori_loop(0, ny // chunk, fields, 0)

    def apply(w, hi, lo):
        a = jnp.dot(w[...], hi, preferred_element_type=F32)
        b = jnp.dot(w[0:ny, :], lo, preferred_element_type=F32)
        return a[0:ny] + a[ny : 2 * ny] + b

    def filter_u(f, carry):
        fu[f] = apply(w_ref, uh[f], ul[f])
        fd[f] = apply(wd_ref, uh[f, :, 0:width], ul[f, :, 0:width])
        return carry

    def filter_x(k, carry):
        fx[k] = apply(w_ref, xh[k], xl[k])
        return carry

    lax.fori_loop(0, 3, filter_u, 0)
    lax.fori_loop(0, 12, filter_x, 0)

    def contract(c, acc):
        r0 = pl.multiple_of(c * chunk, chunk)
        rows = pl.ds(r0, chunk)
        v = [fu[f, rows, :] for f in range(3)]
        g = [fd[f, rows, :] for f in range(3)]
        dx = [half_diff(shifts_x(a, nz))[:, :width] for a in v]
        v = [a[:, :width] for a in v]
        dz = [half_diff(shifts_z(a, nz)) for a in v]
        s = (
            dx[0],
            g[1],
            dz[2],
            0.5 * (g[0] + dx[1]),
            0.5 * (dz[0] + dx[2]),
            0.5 * (dz[1] + g[2]),
        )
        four = 4.0 * norm_of(s)
        lm, mm = [], []
        for k, (i, j) in enumerate(PAIRS):
            leonard = fx[k, rows, :] - v[i] * v[j]
            for t in range(per):
                back[t, k, rows, :] = leonard[:, t * LANES : (t + 1) * LANES]
            model = fx[6 + k, rows, :] - four * s[k]
            weighted = model if k < 3 else 2.0 * model
            lm.append(weighted * leonard)
            mm.append(weighted * model)
        lm = jnp.sum(sum(lm[1:], lm[0]), axis=1, keepdims=True)
        mm = jnp.sum(sum(mm[1:], mm[0]), axis=1, keepdims=True)
        lane = iota((chunk, 2 * NBIN), 1)
        mine = bin_ref[rows, :] == lane % NBIN
        part = jnp.where(mine, jnp.where(lane < NBIN, lm, mm), 0.0)
        for r in range(chunk // 8):
            acc = acc + part[8 * r : 8 * r + 8]
        return acc

    sums = lax.fori_loop(0, ny // chunk, contract, jnp.zeros((8, 2 * NBIN), F32))

    for m in range(n):
        row = pl.multiple_of((me ^ m) * planes, 8)
        for t in range(per):
            for k in range(7):
                o = (t * 7 + k) * planes
                outs[m][o : o + planes, :] = back[t, k, pl.ds(row, planes), :]
        outs[m][per * 7 * planes : per * 7 * planes + 8, :] = sums


def totals_kernel(*refs):
    out = refs[-1]
    total = refs[0][...]
    for r in refs[1:-1]:
        total = total + r[...]
    out[...] = total


def unpack_kernel(n, nz, per, me_ref, *refs):
    ins, refs = refs[:n], refs[n:]
    leonard_ref, mag_ref, tiles = refs
    group = LANES // nz
    nl = 8 // group
    me = me_ref[0]
    planes = mag_ref.shape[0]
    rows = 7 * planes
    for m in range(n):
        d = me ^ m
        for i in range(per):
            t = per * d + i
            tiles[t // nl, t % nl] = ins[m][i * rows : (i + 1) * rows, :]
    for c in range(7):
        for k in range(planes // 8):
            r0 = c * planes + 8 * k
            ts = swap_rows([tiles[:, l, r0 : r0 + 8, :].reshape(LANES, LANES) for l in range(nl)], nz)
            for g in range(nl):
                v = swap_chunks(ts[g], nz).T.reshape(group, nz, LANES)
                p0 = 8 * k + g * group
                if c < 6:
                    leonard_ref[c, p0 : p0 + group] = v
                else:
                    mag_ref[p0 : p0 + group] = v


def viscosity_kernel(cells, me_ref, own_ref, bin_col_ref, bin_row_ref, mag_ref, visc_ref, coef_ref):
    planes = mag_ref.shape[0]
    ny = bin_col_ref.shape[0]
    total = jnp.sum(own_ref[...], axis=0, keepdims=True)
    num = total[:, 0:NBIN]
    den = total[:, NBIN : 2 * NBIN]
    per_bin = num / jnp.maximum(den, F32(cells))
    row = pl.multiple_of(me_ref[0] * planes, 8)
    mine = bin_col_ref[pl.ds(row, planes), :] == iota((planes, NBIN), 1)
    local = jnp.sum(jnp.where(mine, per_bin, 0.0), axis=1, keepdims=True)
    for a in range(planes):
        visc_ref[a] = mag_ref[a] * local[a : a + 1, :]
    eye = iota((NBIN, NBIN), 0) == iota((NBIN, NBIN), 1)
    col = jnp.sum(jnp.where(eye, per_bin, 0.0), axis=1, keepdims=True)
    hit = bin_row_ref[...] == iota((NBIN, ny), 0)
    coef_ref[...] = jnp.sum(jnp.where(hit, col, 0.0), axis=0, keepdims=True)


def local(npx, n, velocity, filter_inverse, filter_block, plane_bin):
    _, planes, nz, nx = velocity.shape
    ny = planes * n
    group = LANES // nz
    nt = LANES // group
    per = nt // n
    width = per * LANES
    wide = width + 4 * nz
    rows = 3 * planes
    smem = pl.BlockSpec(memory_space=pltpu.SMEM)
    me = lax.axis_index("pz").astype(jnp.int32).reshape(1)
    bin_col = plane_bin.reshape(ny, 1)
    bin_row = plane_bin.reshape(1, ny)

    w, wd = pl.pallas_call(
        weights_kernel,
        out_shape=[jax.ShapeDtypeStruct((2 * ny, ny), BF16)] * 2,
        in_specs=vmem(3),
        out_specs=vmem(2),
        name="weights",
    )(filter_inverse, filter_block.reshape(ny, 1), filter_block.reshape(1, ny))

    tiles, edges = pl.pallas_call(
        functools.partial(tiles_kernel, nz),
        out_shape=[
            jax.ShapeDtypeStruct((16, 8 // group, rows, LANES), F32),
            jax.ShapeDtypeStruct((2, rows, LANES), F32),
        ],
        in_specs=vmem(1),
        out_specs=vmem(2),
        name="tiles",
    )(velocity)
    if npx == 2:
        other = lax.ppermute(edges, "px", [(0, 1), (1, 0)])
        after, before = other[0], other[1]
    else:
        after = lax.ppermute(edges[0], "px", [((i + 1) % npx, i) for i in range(npx)])
        before = lax.ppermute(edges[1], "px", [(i, (i + 1) % npx) for i in range(npx)])
    blocks = pl.pallas_call(
        functools.partial(blocks_kernel, n, nz),
        out_shape=[jax.ShapeDtypeStruct((rows, wide), F32)] * n,
        in_specs=[smem] + vmem(3),
        out_specs=vmem(n),
        name="blocks",
    )(me, tiles.reshape(nt, rows, LANES), after, before)

    order = sorted(range(1, n), key=lambda m: (m & 3 == 0, -m))

    def exchange(arrays):
        got = [arrays[0]] + [None] * (n - 1)
        for m in order:
            got[m] = lax.ppermute(arrays[m], "pz", [(i, i ^ m) for i in range(n)])
        return got

    columns = exchange(blocks)
    tall = per * 7 * planes + 8
    results = pl.pallas_call(
        functools.partial(column_kernel, n, nz, width),
        out_shape=[jax.ShapeDtypeStruct((tall, LANES), F32)] * n,
        in_specs=[smem] + vmem(n + 3),
        out_specs=vmem(n),
        scratch_shapes=[
            pltpu.VMEM((3, ny + 16, wide), F32),
            pltpu.VMEM((3, ny, wide), BF16),
            pltpu.VMEM((3, ny, wide), BF16),
            pltpu.VMEM((12, ny, width), BF16),
            pltpu.VMEM((12, ny, width), BF16),
            pltpu.VMEM((3, ny, wide), F32),
            pltpu.VMEM((3, ny, width), F32),
            pltpu.VMEM((12, ny, width), F32),
            pltpu.VMEM((per, 7, ny, LANES), F32),
        ],
        name="columns",
    )(me, *columns, w, wd, bin_col)

    returned = exchange(results)
    sums = pl.pallas_call(
        totals_kernel,
        out_shape=jax.ShapeDtypeStruct((8, LANES), F32),
        grid=(1,),
        in_specs=[pl.BlockSpec((8, LANES), lambda i: (tall // 8 - 1, 0))] * n,
        out_specs=pl.BlockSpec((8, LANES), lambda i: (0, 0)),
        name="totals",
    )(*returned)
    step = 1
    while step < npx:
        sums = sums + lax.ppermute(sums, "px", [(i, i ^ step) for i in range(npx)])
        step *= 2
    leonard, magnitude = pl.pallas_call(
        functools.partial(unpack_kernel, n, nz, per),
        out_shape=[
            jax.ShapeDtypeStruct((6, planes, nz, nx), F32),
            jax.ShapeDtypeStruct((planes, nz, nx), F32),
        ],
        in_specs=[smem] + vmem(n),
        out_specs=vmem(2),
        scratch_shapes=[pltpu.VMEM((16, 8 // group, 7 * planes, LANES), F32)],
        name="unpack",
    )(me, *returned)
    viscosity, coefficient = pl.pallas_call(
        functools.partial(viscosity_kernel, nx * npx * nz),
        out_shape=[
            jax.ShapeDtypeStruct((planes, nz, nx), F32),
            jax.ShapeDtypeStruct((1, ny), F32),
        ],
        in_specs=[smem] + vmem(4),
        out_specs=vmem(2),
        name="viscosity",
    )(me, sums, bin_col, bin_row, magnitude)
    return leonard, viscosity, coefficient.reshape(ny)


def solution(mesh):
    return jax.shard_map(
        functools.partial(local, mesh.shape["px"], mesh.shape["pz"]),
        mesh=mesh,
        in_specs=(P(None, "pz", None, "px"), P(), P(), P()),
        out_specs=(P(None, "pz", None, "px"), P("pz", None, "px"), P()),
        check_vma=False,
    )
```

```python
import functools

import jax
import jax.numpy as jnp
from jax import lax
from jax.experimental import pallas as pl
from jax.experimental.pallas import tpu as pltpu
from jax.sharding import PartitionSpec as P

NBIN = 64
LANES = 128
F32 = jnp.float32
BF16 = jnp.bfloat16
PAIRS = ((0, 0), (1, 1), (2, 2), (0, 1), (0, 2), (1, 2))


def vmem(n):
    return [pl.BlockSpec(memory_space=pltpu.VMEM)] * n


def iota(shape, dim):
    return lax.broadcasted_iota(jnp.int32, shape, dim)


def swap_chunks(t, nz):
    group = LANES // nz
    rows, cols = t.shape
    row, lane = iota(t.shape, 0), iota(t.shape, 1)
    bit = group // 2
    while bit:
        up = pltpu.roll(pltpu.roll(t, bit * nz, 1), rows - bit, 0)
        down = pltpu.roll(pltpu.roll(t, cols - bit * nz, 1), bit, 0)
        rbit = (row // bit) % 2
        lbit = (lane // (bit * nz)) % 2
        t = jnp.where(rbit == lbit, t, jnp.where(rbit == 0, up, down))
        bit //= 2
    return t


def swap_rows(ts, nz):
    group = LANES // nz
    ts = list(ts)
    rows = ts[0].shape[0]
    row = iota(ts[0].shape, 0)
    bit = len(ts) // 2
    while bit:
        low = (row // (bit * group)) % 2 == 0
        for g in range(len(ts)):
            if not g & bit:
                a, b = ts[g], ts[g | bit]
                ts[g] = jnp.where(low, a, pltpu.roll(b, bit * group, 0))
                ts[g | bit] = jnp.where(low, pltpu.roll(a, rows - bit * group, 0), b)
        bit //= 2
    return ts


def tiles_kernel(nz, vel_ref, out_ref, edge_ref):
    group = LANES // nz
    nl = 8 // group
    planes = vel_ref.shape[1]
    for f in range(3):
        for k in range(planes // 8):
            ts = []
            for g in range(nl):
                p0 = 8 * k + g * group
                v = vel_ref[f, p0 : p0 + group].reshape(LANES, LANES)
                ts.append(swap_chunks(v.T, nz))
            ts = swap_rows(ts, nz)
            r0 = f * planes + 8 * k
            for l in range(nl):
                t = ts[l].reshape(16, 8, LANES)
                out_ref[:, l, r0 : r0 + 8, :] = t
                if l == 0:
                    edge_ref[0, r0 : r0 + 8, :] = t[0]
                if l == nl - 1:
                    edge_ref[1, r0 : r0 + 8, :] = t[15]


def blocks_kernel(n, nz, me_ref, tiles_ref, edge_ref, *outs):
    group = LANES // nz
    nt = LANES // group
    per = nt // n
    me = me_ref[0]
    rows = tiles_ref.shape[1]
    lane = iota((rows, LANES), 1)
    for m in range(n):
        d = me ^ m
        for i in range(per):
            outs[m][:, i * LANES : (i + 1) * LANES] = tiles_ref[per * d + i]
        after = jnp.minimum(per * d + per, nt - 1)
        before = jnp.maximum(per * d - 1, 0)
        right = jnp.where(d == n - 1, edge_ref[0], tiles_ref[after])
        left = jnp.where(d == 0, edge_ref[1], tiles_ref[before])
        c0 = per * LANES
        if group == 4:
            outs[m][:, c0 : c0 + LANES] = jnp.where(lane < 2 * nz, right, left)
        else:
            outs[m][:, c0 : c0 + LANES] = right
            outs[m][:, c0 + LANES : c0 + 2 * LANES] = left


def split(x):
    hi = x.astype(BF16)
    lo = (x - hi.astype(F32)).astype(BF16)
    return hi, lo


def weights_kernel(nz, inv_ref, col_ref, row_ref, w_ref, wd_ref, box_ref):
    ny = inv_ref.shape[0]
    masked = jnp.where(col_ref[...] == row_ref[...], inv_ref[...], 0.0)
    w = masked / jnp.sum(masked, axis=1, keepdims=True)
    hi, lo = split(w)
    w_ref[0:ny] = hi
    w_ref[ny : 2 * ny] = lo
    lane = iota((ny, ny), 1)
    before = jnp.where(lane == 0, 0.0, pltpu.roll(w, 1, 1))
    after = jnp.where(lane == ny - 1, 0.0, pltpu.roll(w, ny - 1, 1))
    hi, lo = split(0.5 * (before - after))
    wd_ref[0:ny] = hi
    wd_ref[ny : 2 * ny] = lo
    wide = box_ref.shape[0]
    chunk = LANES
    for c in range(wide // chunk):
        source = iota((chunk, wide), 0) + c * chunk
        target = iota((chunk, wide), 1)

        def tap(a, b, size):
            gap = jnp.abs(a - b)
            near = (gap == 1) | (gap == size - 1)
            return jnp.where(gap == 0, 0.5, jnp.where(near, 0.25, 0.0))

        in_x = tap(source // nz, target // nz, wide // nz)
        in_z = tap(source % nz, target % nz, nz)
        box_ref[c * chunk : (c + 1) * chunk, :] = (in_x * in_z).astype(BF16)


def shifts_z(v, nz):
    width = v.shape[1]
    z = iota(v.shape, 1) % nz
    below = jnp.where(z == 0, pltpu.roll(v, width - (nz - 1), 1), pltpu.roll(v, 1, 1))
    above = jnp.where(z == nz - 1, pltpu.roll(v, nz - 1, 1), pltpu.roll(v, width - 1, 1))
    return below, above


def shifts_x(v, nz):
    width = v.shape[1]
    return pltpu.roll(v, nz, 1), pltpu.roll(v, width - nz, 1)


def half_diff(pair):
    return 0.5 * (pair[1] - pair[0])


def strain_of(dx, dy, dz):
    return (
        dx[0],
        dy[1],
        dz[2],
        0.5 * (dy[0] + dx[1]),
        0.5 * (dz[0] + dx[2]),
        0.5 * (dz[1] + dy[2]),
    )


def norm_of(s):
    return jnp.sqrt(
        2.0 * (s[0] * s[0] + s[1] * s[1] + s[2] * s[2]) + 4.0 * (s[3] * s[3] + s[4] * s[4] + s[5] * s[5])
    )


def magnitude_kernel(nz, vel_ref, below_ref, above_ref, edge_ref, mag_ref):
    planes = vel_ref.shape[1]
    rows = edge_ref.shape[1]
    zeros = jnp.zeros((LANES - rows, LANES), F32)
    right = jnp.concatenate([edge_ref[0], zeros], axis=0).T[0:nz]
    left = jnp.concatenate([edge_ref[1], zeros], axis=0).T[LANES - nz : LANES]
    lane = iota((nz, LANES), 1)
    for a in range(planes):
        dx, dy, dz = [], [], []
        for f in range(3):
            v = vel_ref[f, a]
            col = f * planes + a
            after = jnp.where(lane == LANES - 1, right[:, col : col + 1], pltpu.roll(v, LANES - 1, 1))
            before = jnp.where(lane == 0, left[:, col : col + 1], pltpu.roll(v, 1, 1))
            dx.append(0.5 * (after - before))
            upper = vel_ref[f, a + 1] if a + 1 < planes else above_ref[f, 0]
            lower = vel_ref[f, a - 1] if a else below_ref[f, 0]
            dy.append(0.5 * (upper - lower))
            dz.append(0.5 * (pltpu.roll(v, nz - 1, 0) - pltpu.roll(v, 1, 0)))
        mag_ref[a] = norm_of(strain_of(dx, dy, dz))


def column_kernel(n, nz, width, me_ref, *refs):
    ins, refs = refs[:n], refs[n:]
    w_ref, wd_ref, box_ref, bin_ref = refs[:4]
    outs, refs = refs[4 : 4 + n], refs[4 + n :]
    u_ref, uh, ul, ph, pl_, fu, fd, fx, back = refs
    me = me_ref[0]
    ny = bin_ref.shape[0]
    planes = ny // n
    wide = u_ref.shape[2]
    per = width // LANES
    pad = 8
    chunk = 16

    for f in range(3):
        u_ref[f, 0:pad, :] = jnp.zeros((pad, wide), F32)
        u_ref[f, ny + pad : ny + 2 * pad, :] = jnp.zeros((pad, wide), F32)
    for m in range(n):
        row = pl.multiple_of((me ^ m) * planes, 8)
        for f in range(3):
            u_ref[f, pl.ds(pad + row, planes), :] = ins[m][f * planes : (f + 1) * planes, :]

    def fields(c, carry):
        r0 = pl.multiple_of(c * chunk, chunk)
        rows = pl.ds(r0, chunk)
        u, dx, dy, dz = [], [], [], []
        for f in range(3):
            ext = u_ref[f, pl.ds(r0, chunk + 2 * pad), :]
            v = ext[pad : pad + chunk]
            u.append(v)
            dy.append(0.5 * (ext[pad + 1 : pad + 1 + chunk] - ext[pad - 1 : pad - 1 + chunk]))
            dx.append(half_diff(shifts_x(v, nz)))
            dz.append(half_diff(shifts_z(v, nz)))
            uh[f, rows, :], ul[f, rows, :] = split(v)
        s = strain_of(dx, dy, dz)
        mag = norm_of(s)
        for k, (i, j) in enumerate(PAIRS):
            ph[k, rows, :], pl_[k, rows, :] = split(u[i] * u[j])
            ph[6 + k, rows, :], pl_[6 + k, rows, :] = split(mag * s[k])
        return carry

    lax.fori_loop(0, ny // chunk, fields, 0)

    def dot(a, b):
        return jnp.dot(a, b, preferred_element_type=F32)

    def apply(w, hi, lo):
        a = dot(w[...], hi)
        return a[0:ny] + a[ny : 2 * ny] + dot(w[0:ny, :], lo)

    def filter_u(f, carry):
        hi, lo = split(dot(uh[f], box_ref[...]) + dot(ul[f], box_ref[...]))
        fu[f] = apply(w_ref, hi, lo)
        fd[f] = apply(wd_ref, hi[:, 0:width], lo[:, 0:width])
        return carry

    def filter_x(k, carry):
        hi, lo = split(dot(ph[k], box_ref[:, 0:width]) + dot(pl_[k], box_ref[:, 0:width]))
        fx[k] = apply(w_ref, hi, lo)
        return carry

    lax.fori_loop(0, 3, filter_u, 0)
    lax.fori_loop(0, 12, filter_x, 0)

    def contract(c, acc):
        r0 = pl.multiple_of(c * chunk, chunk)
        rows = pl.ds(r0, chunk)
        v = [fu[f, rows, :] for f in range(3)]
        dy = [fd[f, rows, :] for f in range(3)]
        dx = [half_diff(shifts_x(a, nz))[:, :width] for a in v]
        v = [a[:, :width] for a in v]
        dz = [half_diff(shifts_z(a, nz)) for a in v]
        s = strain_of(dx, dy, dz)
        four = 4.0 * norm_of(s)
        lm, mm = [], []
        for k, (i, j) in enumerate(PAIRS):
            leonard = fx[k, rows, :] - v[i] * v[j]
            for t in range(per):
                back[t, k, rows, :] = leonard[:, t * LANES : (t + 1) * LANES]
            model = fx[6 + k, rows, :] - four * s[k]
            weighted = model if k < 3 else 2.0 * model
            lm.append(weighted * leonard)
            mm.append(weighted * model)
        lm = jnp.sum(sum(lm[1:], lm[0]), axis=1, keepdims=True)
        mm = jnp.sum(sum(mm[1:], mm[0]), axis=1, keepdims=True)
        lane = iota((chunk, 2 * NBIN), 1)
        mine = bin_ref[rows, :] == lane % NBIN
        part = jnp.where(mine, jnp.where(lane < NBIN, lm, mm), 0.0)
        for r in range(chunk // 8):
            acc = acc + part[8 * r : 8 * r + 8]
        return acc

    sums = lax.fori_loop(0, ny // chunk, contract, jnp.zeros((8, 2 * NBIN), F32))

    for m in range(n):
        row = pl.multiple_of((me ^ m) * planes, 8)
        for t in range(per):
            for k in range(6):
                o = (t * 6 + k) * planes
                outs[m][o : o + planes, :] = back[t, k, pl.ds(row, planes), :]
        outs[m][per * 6 * planes : per * 6 * planes + 8, :] = sums


def totals_kernel(*refs):
    out = refs[-1]
    rows = refs[0].shape[0]
    total = refs[0][rows - 8 : rows, :]
    for r in refs[1:-1]:
        total = total + r[rows - 8 : rows, :]
    out[...] = total


def unpack_kernel(n, nz, per, me_ref, *refs):
    ins, (out_ref, tiles) = refs[:n], refs[n:]
    group = LANES // nz
    nl = 8 // group
    me = me_ref[0]
    planes = out_ref.shape[1]
    c = pl.program_id(0)
    for m in range(n):
        d = me ^ m
        for i in range(per):
            t = per * d + i
            row = pl.multiple_of((i * 6 + c) * planes, 8)
            tiles[t // nl, t % nl] = ins[m][pl.ds(row, planes), :]
    for k in range(planes // 8):
        ts = swap_rows([tiles[:, l, 8 * k : 8 * k + 8, :].reshape(LANES, LANES) for l in range(nl)], nz)
        for g in range(nl):
            p0 = 8 * k + g * group
            out_ref[0, p0 : p0 + group] = swap_chunks(ts[g], nz).T.reshape(group, nz, LANES)


def viscosity_kernel(cells, me_ref, own_ref, other_ref, bin_col_ref, bin_row_ref, mag_ref, visc_ref, coef_ref):
    planes = mag_ref.shape[0]
    ny = bin_col_ref.shape[0]
    total = jnp.sum(own_ref[...] + other_ref[...], axis=0, keepdims=True)
    num = total[:, 0:NBIN]
    den = total[:, NBIN : 2 * NBIN]
    per_bin = num / jnp.maximum(den, F32(cells))
    row = pl.multiple_of(me_ref[0] * planes, 8)
    mine = bin_col_ref[pl.ds(row, planes), :] == iota((planes, NBIN), 1)
    local = jnp.sum(jnp.where(mine, per_bin, 0.0), axis=1, keepdims=True)
    for a in range(planes):
        visc_ref[a] = mag_ref[a] * local[a : a + 1, :]
    eye = iota((NBIN, NBIN), 0) == iota((NBIN, NBIN), 1)
    col = jnp.sum(jnp.where(eye, per_bin, 0.0), axis=1, keepdims=True)
    hit = bin_row_ref[...] == iota((NBIN, ny), 0)
    coef_ref[...] = jnp.sum(jnp.where(hit, col, 0.0), axis=0, keepdims=True)


def mib(n):
    return pltpu.CompilerParams(vmem_limit_bytes=n << 20)


def local(npx, n, velocity, filter_inverse, filter_block, plane_bin):
    _, planes, nz, nx = velocity.shape
    ny = planes * n
    group = LANES // nz
    nt = LANES // group
    per = nt // n
    width = per * LANES
    wide = width + 4 * nz
    rows = 3 * planes
    smem = pl.BlockSpec(memory_space=pltpu.SMEM)
    me = lax.axis_index("pz").astype(jnp.int32).reshape(1)
    bin_col = plane_bin.reshape(ny, 1)
    bin_row = plane_bin.reshape(1, ny)

    tiles, edges = pl.pallas_call(
        functools.partial(tiles_kernel, nz),
        out_shape=[
            jax.ShapeDtypeStruct((16, 8 // group, rows, LANES), F32),
            jax.ShapeDtypeStruct((2, rows, LANES), F32),
        ],
        in_specs=vmem(1),
        out_specs=vmem(2),
        compiler_params=mib(6),
        name="tiles",
    )(velocity)
    if npx == 2:
        edges = lax.ppermute(edges, "px", [(0, 1), (1, 0)])
    else:
        after = lax.ppermute(edges[0], "px", [((i + 1) % npx, i) for i in range(npx)])
        before = lax.ppermute(edges[1], "px", [(i, (i + 1) % npx) for i in range(npx)])
        edges = jnp.stack([after, before])
    blocks = pl.pallas_call(
        functools.partial(blocks_kernel, n, nz),
        out_shape=[jax.ShapeDtypeStruct((rows, wide), F32)] * n,
        in_specs=[smem] + vmem(2),
        out_specs=vmem(n),
        compiler_params=mib(6),
        name="blocks",
    )(me, tiles.reshape(nt, rows, LANES), edges)

    def late(m):
        low = m & 3
        return (-max(m.bit_length(), 2), low == 0, bin(low).count("1"), m)

    def exchange(arrays):
        got = [arrays[0]] + [None] * (n - 1)
        for m in sorted(range(1, n), key=late):
            got[m] = lax.ppermute(arrays[m], "pz", [(i, i ^ m) for i in range(n)])
        return got

    columns = exchange(blocks)
    w, wd, box = pl.pallas_call(
        functools.partial(weights_kernel, nz),
        out_shape=[jax.ShapeDtypeStruct((2 * ny, ny), BF16)] * 2 + [jax.ShapeDtypeStruct((wide, wide), BF16)],
        in_specs=vmem(3),
        out_specs=vmem(3),
        compiler_params=mib(6),
        name="weights",
    )(filter_inverse, filter_block.reshape(ny, 1), filter_block.reshape(1, ny))
    tall = per * 6 * planes + 8
    results = pl.pallas_call(
        functools.partial(column_kernel, n, nz, width),
        out_shape=[jax.ShapeDtypeStruct((tall, LANES), F32)] * n,
        in_specs=[smem] + vmem(n + 4),
        out_specs=vmem(n),
        scratch_shapes=[
            pltpu.VMEM((3, ny + 16, wide), F32),
            pltpu.VMEM((3, ny, wide), BF16),
            pltpu.VMEM((3, ny, wide), BF16),
            pltpu.VMEM((12, ny, wide), BF16),
            pltpu.VMEM((12, ny, wide), BF16),
            pltpu.VMEM((3, ny, wide), F32),
            pltpu.VMEM((3, ny, width), F32),
            pltpu.VMEM((12, ny, width), F32),
            pltpu.VMEM((per, 6, ny, LANES), F32),
        ],
        compiler_params=mib(32),
        name="columns",
    )(me, *columns, w, wd, box, bin_col)

    returned = exchange(results)
    upper = lax.slice_in_dim(velocity, 0, 1, axis=1)
    lower = lax.slice_in_dim(velocity, planes - 1, planes, axis=1)
    above = lax.ppermute(upper, "pz", [(i + 1, i) for i in range(n - 1)])
    below = lax.ppermute(lower, "pz", [(i, i + 1) for i in range(n - 1)])
    magnitude = pl.pallas_call(
        functools.partial(magnitude_kernel, nz),
        out_shape=jax.ShapeDtypeStruct((planes, nz, nx), F32),
        in_specs=vmem(4),
        out_specs=vmem(1)[0],
        compiler_params=mib(6),
        name="magnitude",
    )(velocity, below, above, edges)
    own = pl.pallas_call(
        totals_kernel,
        out_shape=jax.ShapeDtypeStruct((8, LANES), F32),
        in_specs=vmem(n),
        out_specs=vmem(1)[0],
        compiler_params=mib(6),
        name="totals",
    )(*returned)
    other = lax.ppermute(own, "px", [(i, i ^ 1) for i in range(npx)])
    step = 2
    while step < npx:
        own = own + other
        other = lax.ppermute(own, "px", [(i, i ^ step) for i in range(npx)])
        step *= 2
    leonard = pl.pallas_call(
        functools.partial(unpack_kernel, n, nz, per),
        grid=(6,),
        out_shape=jax.ShapeDtypeStruct((6, planes, nz, nx), F32),
        in_specs=[smem] + vmem(n),
        out_specs=pl.BlockSpec((1, planes, nz, nx), lambda c: (c, 0, 0, 0)),
        scratch_shapes=[pltpu.VMEM((16, 8 // group, planes, LANES), F32)],
        compiler_params=mib(8),
        name="unpack",
    )(me, *returned)
    viscosity, coefficient = pl.pallas_call(
        functools.partial(viscosity_kernel, nx * npx * nz),
        out_shape=[
            jax.ShapeDtypeStruct((planes, nz, nx), F32),
            jax.ShapeDtypeStruct((1, ny), F32),
        ],
        in_specs=[smem] + vmem(5),
        out_specs=vmem(2),
        compiler_params=mib(4),
        name="viscosity",
    )(me, own, other, bin_col, bin_row, magnitude)
    return leonard, viscosity, coefficient.reshape(ny)


def solution(mesh):
    return jax.shard_map(
        functools.partial(local, mesh.shape["px"], mesh.shape["pz"]),
        mesh=mesh,
        in_specs=(P(None, "pz", None, "px"), P(), P(), P()),
        out_specs=(P(None, "pz", None, "px"), P("pz", None, "px"), P()),
        check_vma=False,
    )
```
